32 devices in a mesh: rep: 8 (over y, x, core), tp: 4 (over z).
Axes of the slice: x: 2, y: 2, z: 4, core: 2. Of those that a mesh axis runs over, the one named last changes fastest.
Arguments:
- states: bfloat16 [4, 32, 8192], P(None, 'rep'), may hold values from -6 to 6
- norm_gain: float32 [8192], replicated, may hold values from 0.1 to 1.9
- w_query: bfloat16 [8192, 8192], P(('rep', 'tp')), may hold values from -0.0625 to 0.0625
- w_key: bfloat16 [8192, 1024], P(('rep', 'tp')), may hold values from -0.0625 to 0.0625
- w_value: bfloat16 [8192, 1024], P(('rep', 'tp')), may hold values from -0.0625 to 0.0625
- w_out: bfloat16 [8192, 8192], P(None, ('rep', 'tp')), may hold values from -0.0625 to 0.0625
- bias_query: bfloat16 [8192], P('tp'), may hold values from -4 to 4
- bias_key: bfloat16 [1024], P('tp'), may hold values from -4 to 4
- bias_value: bfloat16 [1024], P('tp'), may hold values from -4 to 4
- key_cache: bfloat16 [32, 8, 4096, 128], P('rep', 'tp'), may hold values from -120 to 120
- value_cache: bfloat16 [32, 8, 4096, 128], P('rep', 'tp'), may hold values from -6 to 6
- lengths: int32 [32], P('rep'), may hold values from 1 to 4096, as said below
Outputs:
- mixed: bfloat16 [4, 32, 8192], P(None, 'rep', 'tp')
The draws below stay inside these ranges and needn't reach their ends.
Inputs may be any that keep to these rules, and one draw needn't show every extreme that they name: `lengths`: each row's number of live cached positions; some row has exactly 4096.
All inputs are finite; a program needn't handle non-finite values.
Results may differ from the reference program's by a relative error of at most 0.0084.
Values may be sent and summed in bfloat16 or wider, within the bound.
A program may use at most 128 MiB of HBM per device.

```python
import jax
import jax.numpy as jnp
from jax import lax

D = 8192
KVH = 8
HS = 128
CTX = 4096
STEPS = 4
KVD = 1024
ROWS = 32


def draw_key_cache(key, part):
    shape = (ROWS, KVH, CTX, HS)
    base = jnp.clip(jax.random.normal(key, shape, jnp.float32), -6.0, 6.0)
    return base.astype(jnp.bfloat16)


def draw_lengths(key, part):
    values = jax.random.randint(key, (ROWS,), 1, CTX + 1)
    chosen = jax.random.randint(jax.random.fold_in(key, 3), (), 0, ROWS)
    return jnp.where(jnp.arange(ROWS) == chosen, CTX, values).astype(jnp.int32)


def steps_of(own_key, shape, pieces, smallest, largest):
    def one(position, blocks):
        steps = jax.random.uniform(jax.random.fold_in(jax.random.fold_in(own_key, 6), position), (blocks,), jnp.float32, smallest / len(pieces), largest / len(pieces))
        return jnp.repeat(jnp.exp(steps), shape[position] // blocks).reshape((-1,) + (1,) * (len(shape) - position - 1))

    loudness = one(*pieces[0])
    for cut in pieces[1:]:
        loudness = loudness * one(*cut)
    return loudness


def noise(stream_key, extent, spread, limit, split=(), kind=jnp.bfloat16):
    loudness = steps_of(stream_key, extent, split, -0.22, 0.18) if split else 1.0
    result = jax.random.normal(stream_key, extent, jnp.float32) * spread * loudness
    return jnp.minimum(jnp.maximum(result, -limit), limit).astype(kind)


def setup_inputs(seed: int = 0) -> dict:
    streams_of = jax.random.split(jax.random.key(seed), 13)
    return {
        "states": noise(streams_of[0], (STEPS, ROWS, D), 1.0, 6.0, ((1, 8),)),
        "norm_gain": jnp.clip(1.0 + 0.18 * jax.random.normal(streams_of[1], (D,), jnp.float32), 0.1, 1.9),
        "w_query": noise(streams_of[2], (D, D), D ** -0.5, 0.0625, ((0, 32),)),
        "w_key": noise(streams_of[3], (D, KVD), D ** -0.5, 0.0625, ((0, 32),)),
        "w_value": noise(streams_of[4], (D, KVD), D ** -0.5, 0.0625, ((0, 32),)),
        "w_out": noise(streams_of[5], (D, D), D ** -0.5, 0.0625, ((1, 32),)),
        "bias_query": noise(streams_of[6], (D,), 1.0, 4.0, ((0, 4),)),
        "bias_key": noise(streams_of[7], (KVD,), 1.0, 4.0, ((0, 4),)),
        "bias_value": noise(streams_of[8], (KVD,), 1.0, 4.0, ((0, 4),)),
        "key_cache": draw_key_cache(jax.random.fold_in(streams_of[12], 71), 0),
        "value_cache": noise(streams_of[10], (ROWS, KVH, CTX, HS), 1.0, 6.0, ((0, 8), (1, 4))),
        "lengths": draw_lengths(jax.random.fold_in(streams_of[12], 71), 0),
    }


THETA = 1000000.0
EPS = 1e-06

def rotate(vectors, positions, head_size):
    half = head_size // 2
    freqs = THETA ** (-jnp.arange(half, dtype=jnp.float32) * 2.0 / head_size)
    angles = positions.astype(jnp.float32)[..., None, None] * freqs
    first = vectors[..., :half]
    second = vectors[..., half:]
    cosine = jnp.cos(angles)
    sine = jnp.sin(angles)
    return jnp.concatenate([first * cosine - second * sine, second * cosine + first * sine], axis=-1)

def reference(states, norm_gain, w_query, w_key, w_value, w_out, bias_query, bias_key, bias_value, key_cache, value_cache, lengths):
    steps, rows, width = states.shape
    heads_kv = key_cache.shape[1]
    head_size = key_cache.shape[3]
    heads_q = width // head_size
    group = heads_q // heads_kv
    flat = states.reshape(steps * rows, width).astype(jnp.float32)
    factor = lax.rsqrt(lax.optimization_barrier(jnp.mean(flat * flat, axis=-1, keepdims=True)) + EPS)
    normed = (flat * factor * norm_gain.astype(jnp.float32)).astype(jnp.bfloat16)
    query = jnp.dot(normed, w_query, preferred_element_type=jnp.float32) + bias_query.astype(jnp.float32)
    keys = jnp.dot(normed, w_key, preferred_element_type=jnp.float32) + bias_key.astype(jnp.float32)
    values = jnp.dot(normed, w_value, preferred_element_type=jnp.float32) + bias_value.astype(jnp.float32)
    positions = lengths.astype(jnp.int32)[None, :] + jnp.arange(steps, dtype=jnp.int32)[:, None]
    query = rotate(query.reshape(steps, rows, heads_q, head_size), positions, head_size).astype(jnp.bfloat16)
    keys = rotate(keys.reshape(steps, rows, heads_kv, head_size), positions, head_size).astype(jnp.bfloat16)
    values = values.reshape(steps, rows, heads_kv, head_size).astype(jnp.bfloat16)
    scale = 1.0 / head_size ** 0.5
    count = steps * group

    def one_row(items):
        row_query, row_keys, row_values, cache_k, cache_v, length = items
        grouped = row_query.reshape(steps, heads_kv, group, head_size).transpose(1, 0, 2, 3)
        grouped = grouped.reshape(heads_kv, count, head_size).astype(jnp.float32)
        old_scores = jnp.einsum('kqh,kch->kqc', grouped, cache_k.astype(jnp.float32)) * scale
        old_valid = (jnp.arange(cache_k.shape[1], dtype=jnp.int32) < length)[None, None, :]
        new_scores = jnp.einsum('kqh,jkh->kqj', grouped, row_keys.astype(jnp.float32)) * scale
        rank = jnp.arange(count, dtype=jnp.int32) // group
        new_valid = (jnp.arange(steps, dtype=jnp.int32)[None, :] <= rank[:, None])[None, :, :]
        scores = jnp.concatenate([old_scores, new_scores], axis=-1)
        valid = jnp.concatenate([jnp.broadcast_to(old_valid, old_scores.shape), jnp.broadcast_to(new_valid, new_scores.shape)], axis=-1)
        scores = jnp.where(valid, scores, -1e+30)
        top = lax.optimization_barrier(jnp.max(scores, axis=-1, keepdims=True))
        weights = jnp.where(valid, jnp.exp(scores - top), 0.0)
        total = lax.optimization_barrier(jnp.sum(weights, axis=-1, keepdims=True))
        rounded = weights.astype(jnp.bfloat16).astype(jnp.float32)
        every_value = jnp.concatenate([cache_v, row_values.transpose(1, 0, 2)], axis=1).astype(jnp.float32)
        attended = jnp.einsum('kqc,kch->kqh', rounded, every_value) / total
        attended = attended.reshape(heads_kv, steps, group, head_size).transpose(1, 0, 2, 3)
        return attended.reshape(steps, width).astype(jnp.bfloat16)
    attended = lax.map(one_row, (query.transpose(1, 0, 2, 3), keys.transpose(1, 0, 2, 3), values.transpose(1, 0, 2, 3), key_cache, value_cache, lengths.astype(jnp.int32)))
    attended = attended.transpose(1, 0, 2).reshape(steps * rows, width)
    mixed = flat + jnp.dot(attended, w_out, preferred_element_type=jnp.float32)
    return mixed.astype(jnp.bfloat16).reshape(steps, rows, width)
```

```python
import functools

import jax
import jax.numpy as jnp
from jax import lax
from jax.experimental import pallas as pl
from jax.experimental.pallas import tpu as pltpu
from jax.sharding import PartitionSpec as P

THETA = 1000000.0
EPS = 1e-06
MESH = pl.DeviceIdType.MESH
BLK = 1024
TILE = 256


def rotate(vectors, positions, head_size):
    half = head_size // 2
    freqs = THETA ** (-jnp.arange(half, dtype=jnp.float32) * 2.0 / head_size)
    angles = positions.astype(jnp.float32)[..., None, None] * freqs
    first = vectors[..., :half]
    second = vectors[..., half:]
    cosine = jnp.cos(angles)
    sine = jnp.sin(angles)
    return jnp.concatenate(
        [first * cosine - second * sine, second * cosine + first * sine], axis=-1
    )


def remote(src, dst, send, recv, device):
    return pltpu.make_async_remote_copy(
        src_ref=src, dst_ref=dst, send_sem=send, recv_sem=recv,
        device_id=device, device_id_type=MESH,
    )


def project_kernel(
    R, T, x_ref, wq_ref, wk_ref, wv_ref, out_ref,
    xs, wbuf, sendp, recvp, own, send2, recv2, send3, recv3,
    wsem, lsem, xsend, xrecv, psend, precv, s2send, s2recv, s3send, s3recv,
):
    r, t = lax.axis_index("rep"), lax.axis_index("tp")
    half = R // 2
    c, q = lax.rem(r, 2), r // 2
    partner = r + 1 - 2 * c
    rows, depth = x_ref.shape[1], x_ref.shape[2]
    qw, kw = wq_ref.shape[1] // T, wk_ref.shape[1] // T
    cw = qw + 2 * kw

    def target(j):
        return lax.rem(t + 1 + j, T)

    loads = []
    for j in range(T):
        d = target(j)
        group = []
        for i, (ref, width, place) in enumerate(
            ((wq_ref, qw, 0), (wk_ref, kw, qw), (wv_ref, kw, qw + kw))
        ):
            group.append(
                pltpu.make_async_copy(
                    ref.at[:, pl.ds(pl.multiple_of(d * width, width), width)],
                    wbuf.at[j, :, pl.ds(place, width)],
                    wsem.at[j, i],
                )
            )
        loads.append(group)
    for group in loads:
        for copy in group:
            copy.start()
    mine = pltpu.make_async_copy(x_ref.at[r], xs.at[c, q], lsem)
    mine.start()

    barrier = pltpu.get_barrier_semaphore()
    for d in range(1, R):
        pl.semaphore_signal(
            barrier, inc=1, device_id=(lax.rem(r + d, R), t), device_id_type=MESH
        )
    for d in range(1, T):
        pl.semaphore_signal(
            barrier, inc=1, device_id=(r, lax.rem(t + d, T)), device_id_type=MESH
        )
    pl.semaphore_wait(barrier, R + T - 2)

    sends = []
    for d in range(1, R):
        peer = lax.rem(r + d, R)
        copy = remote(x_ref.at[peer], xs.at[c, q], xsend.at[d], xrecv.at[d], (peer, t))
        copy.start()
        sends.append(copy)
    mine.wait()
    for d in range(1, R):
        source = lax.rem(r + R - d, R)
        slot = xs.at[lax.rem(source, 2), source // 2]
        remote(slot, slot, xsend.at[d], xrecv.at[d], (source, t)).wait_recv()

    def first(j):
        for copy in loads[j]:
            copy.wait()

        def tile(i, _):
            cols = pl.ds(pl.multiple_of(i * TILE, TILE), TILE)
            w = wbuf[j, :, cols]
            away = jnp.dot(
                xs[1 - c].reshape(half * rows, depth), w, preferred_element_type=jnp.float32
            )
            sendp[j, :, :, cols] = away.astype(jnp.bfloat16).reshape(half, rows, TILE)
            here = jnp.dot(
                xs[c].reshape(half * rows, depth), w, preferred_element_type=jnp.float32
            )
            own[j, :, :, cols] = here.reshape(half, rows, TILE)
            return 0

        lax.fori_loop(0, cw // TILE, tile, 0)
        copy = remote(sendp.at[j], recvp.at[j], psend.at[j], precv.at[j], (partner, t))
        copy.start()
        sends.append(copy)

    def second(j):
        remote(sendp.at[j], recvp.at[j], psend.at[j], precv.at[j], (partner, t)).wait_recv()
        both = own[j] + recvp[j].astype(jnp.float32)
        own[j] = both
        send2[j] = both.astype(jnp.bfloat16)
        for d in range(1, half):
            to = lax.rem(q + d, half)
            copy = remote(
                send2.at[j, to], recv2.at[j, d], s2send.at[j, d], s2recv.at[j, d], (2 * to + c, t)
            )
            copy.start()
            sends.append(copy)

    def third(j):
        total = own[j, q]
        for d in range(1, half):
            slot = recv2.at[j, d]
            remote(slot, slot, s2send.at[j, d], s2recv.at[j, d], (partner, t)).wait_recv()
            total += slot[...].astype(jnp.float32)
        if j < T - 1:
            send3[j] = total.astype(jnp.bfloat16)
            copy = remote(
                send3.at[j], recv3.at[j], s3send.at[j], s3recv.at[j], (r, target(j))
            )
            copy.start()
            sends.append(copy)
        else:
            out_ref[...] = total

    for step in range(T + 3):
        if step < T:
            first(step)
        if 1 <= step <= T:
            second(step - 1)
        if 3 <= step:
            third(step - 3)
    for j in range(T - 1):
        slot = recv3.at[j]
        remote(slot, slot, s3send.at[j], s3recv.at[j], (partner, t)).wait_recv()
        out_ref[...] += slot[...].astype(jnp.float32)
    for copy in sends:
        copy.wait_send()


def project(R, T, x, w_query, w_key, w_value):
    _, rows, depth = x.shape
    cw = (w_query.shape[1] + w_key.shape[1] + w_value.shape[1]) // T
    half = R // 2
    bf, f32 = jnp.bfloat16, jnp.float32
    dma = pltpu.SemaphoreType.DMA
    any_spec = pl.BlockSpec(memory_space=pl.ANY)
    vmem = pl.BlockSpec(memory_space=pltpu.VMEM)
    return pl.pallas_call(
        functools.partial(project_kernel, R, T),
        out_shape=jax.ShapeDtypeStruct((rows, cw), f32),
        in_specs=[vmem, any_spec, any_spec, any_spec],
        out_specs=vmem,
        scratch_shapes=[
            pltpu.VMEM((2, half, rows, depth), bf),
            pltpu.VMEM((T, depth, cw), bf),
            pltpu.VMEM((T, half, rows, cw), bf),
            pltpu.VMEM((T, half, rows, cw), bf),
            pltpu.VMEM((T, half, rows, cw), f32),
            pltpu.VMEM((T, half, rows, cw), bf),
            pltpu.VMEM((T, half, rows, cw), bf),
            pltpu.VMEM((T, rows, cw), bf),
            pltpu.VMEM((T, rows, cw), bf),
            dma((T, 3)), dma, dma((R,)), dma((R,)), dma((T,)), dma((T,)),
            dma((T, half)), dma((T, half)), dma((T,)), dma((T,)),
        ],
        compiler_params=pltpu.CompilerParams(
            collective_id=0, has_side_effects=True, vmem_limit_bytes=48 << 20
        ),
        name="project",
    )(x, w_query, w_key, w_value)


def attend_kernel(steps, len_ref, q_ref, nk_ref, nv_ref, k_ref, v_ref, o_ref, top, total, accum):
    s = pl.program_id(1)
    length = len_ref[pl.program_id(0)]
    heads, count, head_size = q_ref.shape[1:]
    group = count // steps
    scale = 1.0 / head_size**0.5
    contract = (((1,), (1,)), ((), ()))

    @pl.when(s == 0)
    def _():
        padded = nk_ref.shape[2]
        rank = lax.broadcasted_iota(jnp.int32, (count, padded), 0) // group
        place = lax.broadcasted_iota(jnp.int32, (count, padded), 1)
        for h in range(heads):
            scores = scale * lax.dot_general(
                q_ref[0, h], nk_ref[0, h], contract, preferred_element_type=jnp.float32
            )
            scores = jnp.where(place <= rank, scores, -1e30)
            peak = jnp.max(scores, axis=-1, keepdims=True)
            weights = jnp.where(place <= rank, jnp.exp(scores - peak), 0.0)
            top[h] = jnp.broadcast_to(peak, top.shape[1:])
            total[h] = jnp.broadcast_to(
                jnp.sum(weights, axis=-1, keepdims=True), total.shape[1:]
            )
            accum[h] = jnp.dot(
                weights.astype(jnp.bfloat16), nv_ref[0, h], preferred_element_type=jnp.float32
            )

    @pl.when(s * k_ref.shape[2] < length)
    def _():
        block = k_ref.shape[2]
        place = s * block + lax.broadcasted_iota(jnp.int32, (count, block), 1)
        valid = place < length
        for h in range(heads):
            scores = scale * lax.dot_general(
                q_ref[0, h], k_ref[0, h], contract, preferred_element_type=jnp.float32
            )
            scores = jnp.where(valid, scores, -1e30)
            before = top[h][:, :1]
            fresh = jnp.maximum(before, jnp.max(scores, axis=-1, keepdims=True))
            weights = jnp.where(valid, jnp.exp(scores - fresh), 0.0)
            factor = jnp.exp(before - fresh)
            top[h] = jnp.broadcast_to(fresh, top.shape[1:])
            total[h] = total[h] * factor + jnp.sum(weights, axis=-1, keepdims=True)
            accum[h] = accum[h] * factor + jnp.dot(
                weights.astype(jnp.bfloat16), v_ref[0, h], preferred_element_type=jnp.float32
            )

    @pl.when(s == pl.num_programs(1) - 1)
    def _():
        for h in range(heads):
            o_ref[0, h] = (accum[h] / total[h]).astype(o_ref.dtype)


def attend(query, new_keys, new_values, key_cache, value_cache, lengths):
    steps, rows, heads_q, head_size = query.shape
    heads, context = key_cache.shape[1:3]
    group = heads_q // heads
    count = steps * group
    grouped = query.reshape(steps, rows, heads, group, head_size).transpose(1, 2, 0, 3, 4)
    grouped = grouped.reshape(rows, heads, count, head_size)
    pad = ((0, 0), (0, 0), (0, -steps % 16), (0, 0))
    fresh_keys = jnp.pad(new_keys.transpose(1, 2, 0, 3), pad)
    fresh_values = jnp.pad(new_values.transpose(1, 2, 0, 3), pad)
    block = min(BLK, context)

    def small(b, s, lens):
        return (b, 0, 0, 0)

    def cache(b, s, lens):
        return (b, 0, jnp.minimum(s, (lens[b] - 1) // block), 0)

    padded = fresh_keys.shape[2]
    attended = pl.pallas_call(
        functools.partial(attend_kernel, steps),
        out_shape=jax.ShapeDtypeStruct((rows, heads, count, head_size), jnp.bfloat16),
        grid_spec=pltpu.PrefetchScalarGridSpec(
            num_scalar_prefetch=1,
            grid=(rows, context // block),
            in_specs=[
                pl.BlockSpec((1, heads, count, head_size), small),
                pl.BlockSpec((1, heads, padded, head_size), small),
                pl.BlockSpec((1, heads, padded, head_size), small),
                pl.BlockSpec((1, heads, block, head_size), cache),
                pl.BlockSpec((1, heads, block, head_size), cache),
            ],
            out_specs=pl.BlockSpec((1, heads, count, head_size), small),
            scratch_shapes=[pltpu.VMEM((heads, count, head_size), jnp.float32)] * 3,
        ),
        compiler_params=pltpu.CompilerParams(
            dimension_semantics=("arbitrary", "arbitrary"), vmem_limit_bytes=32 << 20
        ),
        name="attend",
    )(lengths, grouped, fresh_keys, fresh_values, key_cache, value_cache)
    attended = attended.reshape(rows, heads, steps, group, head_size).transpose(2, 0, 1, 3, 4)
    return attended.reshape(steps * rows, heads_q * head_size)


def output_kernel(
    R, T, a_ref, w_ref, out_ref, att, wbuf, acc, obuf, orecv,
    wsem, lsem, zsend, zrecv, csend, crecv, psend, precv, osend, orsem,
):
    r, t = lax.axis_index("rep"), lax.axis_index("tp")
    half, m = R // 2, R // T
    c, q = lax.rem(r, 2), r // 2
    partner = r + 1 - 2 * c
    rows, qw = a_ref.shape
    depth = w_ref.shape[1]
    block = r // m
    slot = lax.rem(r, m) * T + t

    def place(j):
        return lax.rem(t + j, T)

    loads = []
    for j in range(T):
        copy = pltpu.make_async_copy(
            w_ref.at[pl.ds(pl.multiple_of(place(j) * qw, qw), qw), :], wbuf.at[j], wsem.at[j]
        )
        copy.start()
        loads.append(copy)
    mine = pltpu.make_async_copy(a_ref, att.at[t, c, q], lsem.at[0])
    mine.start()

    barrier = pltpu.get_barrier_semaphore()
    for d in range(1, R * T):
        index = lax.rem(r * T + t + d, R * T)
        pl.semaphore_signal(
            barrier, inc=1, device_id=(index // T, lax.rem(index, T)), device_id_type=MESH
        )
    pl.semaphore_wait(barrier, R * T - 1)

    sends = []

    def begin(copy):
        copy.start()
        sends.append(copy)

    for d in range(1, T):
        begin(remote(a_ref, att.at[t, c, q], zsend.at[d], zrecv.at[d], (r, place(d))))
    mine.wait()
    order = [0] + [k for pair in zip(range(T - 1, 0, -1), range(1, T)) for k in pair]
    order = list(dict.fromkeys(order))
    for j in order:
        piece = att.at[place(j), c, q]
        if j:
            d = T - j
            remote(piece, piece, zsend.at[d], zrecv.at[d], (r, place(j))).wait_recv()
        for e in range(1, half):
            to = lax.rem(q + e, half)
            begin(remote(piece, piece, csend.at[j, e], crecv.at[j, e], (2 * to + c, t)))
    for j in order:
        for e in range(1, half):
            piece = att.at[place(j), c, lax.rem(q + half - e, half)]
            remote(piece, piece, csend.at[j, e], crecv.at[j, e], (partner, t)).wait_recv()
        whole = att.at[place(j), c]
        begin(remote(whole, whole, psend.at[j], precv.at[j], (partner, t)))
    for n, j in enumerate(order):
        other = att.at[place(j), 1 - c]
        remote(other, other, psend.at[j], precv.at[j], (partner, t)).wait_recv()
        loads[j].wait()
        part = jnp.dot(
            att[place(j)].reshape(R * rows, qw), wbuf[j], preferred_element_type=jnp.float32
        )
        if n:
            acc[...] += part
        else:
            acc[...] = part
    obuf[...] = acc[...].astype(jnp.bfloat16).reshape(R, rows, depth)
    for d in range(1, R):
        to = lax.rem(r + d, R)
        row = lax.rem(to, 2) * half + to // 2
        begin(remote(obuf.at[row], orecv.at[slot], osend.at[d], orsem.at[slot], (to, block)))
    row = c * half + q

    @pl.when(block == t)
    def _():
        copy = pltpu.make_async_copy(obuf.at[row], orecv.at[slot], orsem.at[slot])
        copy.start()

    @pl.when(block != t)
    def _():
        copy = remote(obuf.at[row], orecv.at[slot], osend.at[0], orsem.at[slot], (r, block))
        copy.start()
        copy.wait_send()

    for s in range(R):
        piece = orecv.at[s]
        pltpu.make_async_copy(piece, piece, orsem.at[s]).wait()
    out_ref[...] = orecv[...]
    for copy in sends:
        copy.wait_send()


def output(R, T, attended, w_out):
    rows, qw = attended.shape
    depth = w_out.shape[1]
    half = R // 2
    bf, f32 = jnp.bfloat16, jnp.float32
    dma = pltpu.SemaphoreType.DMA
    vmem = pl.BlockSpec(memory_space=pltpu.VMEM)
    return pl.pallas_call(
        functools.partial(output_kernel, R, T),
        out_shape=jax.ShapeDtypeStruct((R, rows, depth), bf),
        in_specs=[vmem, pl.BlockSpec(memory_space=pl.ANY)],
        out_specs=vmem,
        scratch_shapes=[
            pltpu.VMEM((T, 2, half, rows, qw), bf),
            pltpu.VMEM((T, qw, depth), bf),
            pltpu.VMEM((R * rows, depth), f32),
            pltpu.VMEM((R, rows, depth), bf),
            pltpu.VMEM((R, rows, depth), bf),
            dma((T,)), dma((1,)), dma((T,)), dma((T,)), dma((T, half)), dma((T, half)),
            dma((T,)), dma((T,)), dma((R,)), dma((R,)),
        ],
        compiler_params=pltpu.CompilerParams(
            collective_id=1, has_side_effects=True, vmem_limit_bytes=48 << 20
        ),
        name="output",
    )(attended, w_out)


def on_device(
    R, T, states, norm_gain, w_query, w_key, w_value, w_out,
    bias_query, bias_key, bias_value, key_cache, value_cache, lengths,
):
    steps, rows, width = states.shape
    head_size = key_cache.shape[3]
    count = steps * rows
    depth = width // (R * T)
    t = lax.axis_index("tp")
    flat = states.reshape(count, width).astype(jnp.float32)
    factor = lax.rsqrt(jnp.mean(flat * flat, axis=-1, keepdims=True) + EPS)
    normed = (flat * factor * norm_gain).astype(jnp.bfloat16)
    blocks = normed.reshape(count, R, T, depth)
    blocks = lax.dynamic_index_in_dim(blocks, t, 2, keepdims=False).transpose(1, 0, 2)
    joined = project(R, T, blocks, w_query, w_key, w_value)
    qw, kw = bias_query.shape[0], bias_key.shape[0]
    bias = jnp.concatenate([bias_query, bias_key, bias_value]).astype(jnp.float32)
    joined = joined + bias
    positions = lengths[None, :] + jnp.arange(steps, dtype=jnp.int32)[:, None]
    heads = joined.reshape(steps, rows, (qw + 2 * kw) // head_size, head_size)
    turned = rotate(heads[:, :, : (qw + kw) // head_size], positions, head_size)
    turned = turned.astype(jnp.bfloat16)
    query = turned[:, :, : qw // head_size]
    keys = turned[:, :, qw // head_size :]
    values = heads[:, :, (qw + kw) // head_size :].astype(jnp.bfloat16)
    attended = attend(query, keys, values, key_cache, value_cache, lengths)
    pieces = output(R, T, attended, w_out)
    summed = pieces.transpose(1, 0, 2).reshape(count, R * depth).astype(jnp.float32)
    residual = lax.dynamic_slice_in_dim(flat, t * summed.shape[1], summed.shape[1], 1)
    return (residual + summed).astype(jnp.bfloat16).reshape(steps, rows, summed.shape[1])


def solution(mesh):
    return jax.shard_map(
        functools.partial(on_device, mesh.shape["rep"], mesh.shape["tp"]),
        mesh=mesh,
        in_specs=(
            P(None, "rep", None), P(), P(("rep", "tp"), None), P(("rep", "tp"), None),
            P(("rep", "tp"), None), P(None, ("rep", "tp")), P("tp"), P("tp"), P("tp"),
            P("rep", "tp", None, None), P("rep", "tp", None, None), P("rep"),
        ),
        out_specs=P(None, "rep", "tp"),
        check_vma=False,
    )
```
